128 devices in a mesh: gx: 4 (over x), gy: 4 (over y), gz: 8 (over z, core).
Axes of the slice: x: 4, y: 4, z: 4, core: 2. Of those that a mesh axis runs over, the one named last changes fastest.
Arguments:
- right_side: float32 [5, 2048, 8, 128], P(None, ('gx', 'gy', 'gz')), may hold values from -6 to 6
- diag_inverse: bfloat16 [5, 2048, 128, 128], P(None, ('gx', 'gy', 'gz')), may hold values from -0.5 to 0.5
- off_blocks: bfloat16 [4, 16384, 128, 128], P(None, ('gx', 'gy', 'gz')), may hold values from -0.375 to 0.375
- live_counts: int32 [5, 128], P(None, ('gx', 'gy', 'gz')), may hold values from 1 to 16, as said below
- source_slot: int32 [4, 16384], P(None, ('gx', 'gy', 'gz')), may hold values from 0 to 15, as said below
- target_owner: int32 [4, 16384], P(None, ('gx', 'gy', 'gz')), may hold values from 0 to 127, as said below
- target_block: int32 [4, 16384], P(None, ('gx', 'gy', 'gz')), may hold values from 16 to 79, as said below
Outputs:
- solution: float32 [5, 2048, 8, 128], P(None, ('gx', 'gy', 'gz'))
The draws below stay inside these ranges and needn't reach their ends.
Inputs may be any that keep to these rules, and one draw needn't show every extreme that they name: `live_counts`: slots at or past a device's count in a level are empty; in every level some device has all 16 slots live. `source_slot`: names a live slot of the issuing device in the same level. `target_owner`: in every level, each device's records go exactly 2 each to 64 distinct owners and none to the others. `target_block`: the level part is later than the record's own level, and the slot is live at the owner in that level.
All inputs are finite; a program needn't handle non-finite values.
Results may differ from the reference program's by a relative error of at most 0.013.
Values sent between devices are 32-bit elements; how exact they have to be, the bound alone decides.
No kernel may reach another device: no remote copies, remote signals or barrier semaphores. Data moves between devices by JAX's collectives and lax.ppermute only.
A program may use at most 64 MiB of HBM per device.

```python
import jax
import jax.numpy as jnp
from jax import lax

B = 128
R = 8
LEVELS = 5
S = 16
CAP = 2
OWNERS = 128
RECS = 128
NBLK = 2048


def routing(key):
    base = jax.random.fold_in(key, 7)
    key_count, key_full, key_perm, key_src, key_level, key_slot = jax.random.split(base, 6)
    counts = jax.random.randint(key_count, (LEVELS, OWNERS), 1, S + 1)
    full_owner = jax.random.randint(key_full, (LEVELS,), 0, OWNERS)
    counts = counts.at[jnp.arange(LEVELS), full_owner].set(S)

    def one_list(sub_key):
        first_key, second_key = jax.random.split(sub_key)
        chosen = jax.random.permutation(first_key, OWNERS)[:OWNERS // 2].astype(jnp.int32)
        whole_list = jnp.repeat(chosen, CAP)
        return whole_list[jax.random.permutation(second_key, RECS)]
    list_keys = jax.random.split(key_perm, (LEVELS - 1) * OWNERS)
    owners = jax.vmap(one_list)(list_keys).reshape(LEVELS - 1, OWNERS, RECS)
    shape = (LEVELS - 1, OWNERS, RECS)
    sources = jax.random.randint(key_src, shape, 0, counts[:-1, :, None])
    lowest = (jnp.arange(LEVELS - 1, dtype=jnp.int32) + 1)[:, None, None]
    target_level = jax.random.randint(key_level, shape, lowest, LEVELS)
    target_slot = jax.random.randint(key_slot, shape, 0, counts[target_level, owners])
    blocks = target_level * S + target_slot
    flat = (LEVELS - 1, OWNERS * RECS)
    return (counts.astype(jnp.int32), sources.reshape(flat).astype(jnp.int32), owners.reshape(flat).astype(jnp.int32), blocks.reshape(flat).astype(jnp.int32))


def draw_live_counts(key, part):
    return routing(key)[0]


def draw_source_slot(key, part):
    return routing(key)[1]


def draw_target_owner(key, part):
    return routing(key)[2]


def draw_target_block(key, part):
    return routing(key)[3]


def block_scale(stream_key, shape, cuts, low, high):
    def one(position, shards_of):
        steps = jax.random.uniform(jax.random.fold_in(jax.random.fold_in(stream_key, 6), position), (shards_of,), jnp.float32, low / len(cuts), high / len(cuts))
        return jnp.repeat(jnp.exp(steps), shape[position] // shards_of).reshape((-1,) + (1,) * (len(shape) - position - 1))

    gain = one(*cuts[0])
    for cut in cuts[1:]:
        gain = gain * one(*cut)
    return gain


def scatter_about(own_key, shape, scale, bound, cuts=(), kind=jnp.bfloat16):
    drawn = scale * jax.random.normal(own_key, shape, jnp.float32)
    if cuts:
        drawn = drawn * block_scale(own_key, shape, cuts, -0.22, 0.18)
    return jnp.clip(drawn, -bound, bound).astype(kind)


def setup_inputs(seed: int = 0) -> dict:
    streams_of = jax.random.split(jax.random.key(seed), 8)
    right_side = scatter_about(streams_of[0], (LEVELS, NBLK, R, B), 1.0, 6.0, ((1, 128),), jnp.float32)
    diag_inverse = scatter_about(streams_of[1], (LEVELS, NBLK, B, B), B ** -0.5, 0.5, ((1, 128),))
    off_blocks = scatter_about(streams_of[2], (LEVELS - 1, OWNERS * RECS, B, B), (2 * B) ** -0.5, 0.375, ((1, 128),))
    live_counts = draw_live_counts(jax.random.fold_in(streams_of[7], 71), 0)
    source_slot = draw_source_slot(jax.random.fold_in(streams_of[7], 71), 0)
    target_owner = draw_target_owner(jax.random.fold_in(streams_of[7], 71), 0)
    target_block = draw_target_block(jax.random.fold_in(streams_of[7], 71), 0)
    return {"right_side": right_side, "diag_inverse": diag_inverse, "off_blocks": off_blocks, "live_counts": live_counts, "source_slot": source_slot, "target_owner": target_owner, "target_block": target_block}


def reference(right_side, diag_inverse, off_blocks, live_counts, source_slot, target_owner, target_block):
    accumulated = jnp.zeros((LEVELS * NBLK, R, B), jnp.float32)
    slot_ids = jnp.arange(S, dtype=jnp.int32)
    solved_all = []
    for level_at in range(LEVELS):
        live = (slot_ids[None, :] < live_counts[level_at][:, None]).reshape(NBLK)
        pending = accumulated[level_at * NBLK:(level_at + 1) * NBLK]
        work_rows = (right_side[level_at] - pending).astype(jnp.bfloat16)
        solved = jnp.einsum('nrb,nbc->nrc', work_rows.astype(jnp.float32), diag_inverse[level_at].astype(jnp.float32))
        solved = jnp.where(live[:, None, None], solved, jnp.float32(0.0))
        solved_all.append(solved)
        if level_at + 1 < LEVELS:
            rounded = solved.astype(jnp.bfloat16).reshape(OWNERS, S, R, B)
            blocks = off_blocks[level_at].reshape(OWNERS, RECS, B, B)
            slot_lists = source_slot[level_at].reshape(OWNERS, RECS)

            def per_owner(items):
                owner_rows, owner_blocks, owner_slots = items
                picked = owner_rows[owner_slots]
                return jnp.einsum('krb,kbc->krc', picked.astype(jnp.float32), owner_blocks.astype(jnp.float32))

            contributions = lax.map(per_owner, (rounded, blocks, slot_lists)).reshape(OWNERS * RECS, R, B)
            owner_ids = target_owner[level_at].astype(jnp.int32)
            targets = target_block[level_at].astype(jnp.int32)
            row_ids = (targets // S) * NBLK + owner_ids * S + targets % S
            accumulated = accumulated.at[row_ids].add(contributions)
    return jnp.stack(solved_all)
```

```python
import functools

import jax
import jax.numpy as jnp
from jax import lax
from jax.experimental import pallas as pl
from jax.experimental.pallas import tpu as pltpu
from jax.sharding import PartitionSpec as P

CAP = 2
CHAINS = 4
CHUNKS = 8
AXES = ("gx", "gy", "gz")


def level_kernel(level, levels, slots, records, packed, *refs):
    first, last = level == 0, level == levels - 1
    refs = list(refs)
    counts = refs.pop(0)
    if not last:
        source, slot_of = refs.pop(0), refs.pop(0)
    if not first:
        labels, arrived = refs.pop(0), refs.pop(0)
        if level > 1:
            acc_in = refs.pop(0)
    rhs_hbm, diag_hbm = refs.pop(0), refs.pop(0)
    if not last:
        off_hbm = refs.pop(0)
    solved = refs.pop(0)
    if not last:
        outgoing = refs.pop(0)
        if not first:
            acc = refs.pop(0)
    elif not first:
        acc = refs.pop()
    rhs, diag, sems = refs.pop(0), refs.pop(0), refs.pop(0)
    rhs_copy = pltpu.make_async_copy(rhs_hbm.at[level], rhs, sems.at[0])
    diag_copy = pltpu.make_async_copy(diag_hbm.at[level], diag, sems.at[1])
    rhs_copy.start()
    diag_copy.start()
    off_copies = []
    if not last:
        off = refs.pop(0)
        span = records // CHUNKS
        for chunk in range(CHUNKS):
            rows = pl.ds(chunk * span, span)
            copy = pltpu.make_async_copy(off_hbm.at[level, rows], off.at[rows], sems.at[2 + chunk])
            copy.start()
            off_copies.append(copy)
    blocks = levels * slots + 1
    if not first:
        if level == 1:
            for chain in range(CHAINS):
                for block in range(level * slots, blocks):
                    acc[chain * blocks + block] = jnp.zeros(acc.shape[1:], jnp.float32)
        else:
            for chain in range(CHAINS):
                for block in range(level * slots, blocks):
                    acc[chain * blocks + block] = acc_in[chain * blocks + block]

        def add(step, carry):
            for chain in range(CHAINS):
                at = step * CHAINS + chain
                row = labels[level - 1, at] + chain * blocks
                acc[row] = acc[row] + arrived[at]
            return carry

        lax.fori_loop(0, packed // CHAINS, add, 0, unroll=16)
    rhs_copy.wait()
    diag_copy.wait()
    for slot in range(slots):
        work = rhs[slot]
        if not first:
            pending = acc[level * slots + slot]
            for chain in range(1, CHAINS):
                pending = pending + acc[chain * blocks + level * slots + slot]
            work = work - pending
        value = jnp.dot(work.astype(jnp.bfloat16), diag[slot], preferred_element_type=jnp.float32)
        solved[slot] = jnp.where(slot < counts[level, 0], value, jnp.float32(0.0))
    if not last:
        for record in range(records):
            if record % span == 0:
                off_copies[record // span].wait()
            picked = solved[source[level, record]].astype(jnp.bfloat16)
            outgoing[slot_of[level, record]] = jnp.dot(
                picked, off[record], preferred_element_type=jnp.float32
            )


def one_level(level, levels, slots, rhs_count, width, records, packed, args):
    first, last = level == 0, level == levels - 1
    smem = pl.BlockSpec(memory_space=pltpu.SMEM)
    vmem = pl.BlockSpec(memory_space=pltpu.VMEM)
    anywhere = pl.BlockSpec(memory_space=pltpu.HBM)
    in_specs = [smem]
    if not last:
        in_specs += [smem, smem]
    aliases = {}
    if not first:
        in_specs += [smem, vmem]
        if level > 1:
            in_specs += [vmem]
    in_specs += [anywhere, anywhere]
    if not last:
        in_specs += [anywhere]
    acc_shape = (CHAINS * (levels * slots + 1), rhs_count, width)
    shapes = [jax.ShapeDtypeStruct((slots, rhs_count, width), jnp.float32)]
    scratch = [
        pltpu.VMEM((slots, rhs_count, width), jnp.float32),
        pltpu.VMEM((slots, width, width), jnp.bfloat16),
        pltpu.SemaphoreType.DMA((2 + CHUNKS,)),
    ]
    if not last:
        shapes += [jax.ShapeDtypeStruct((packed, rhs_count, width), jnp.float32)]
        if not first:
            shapes += [jax.ShapeDtypeStruct(acc_shape, jnp.float32)]
        scratch += [pltpu.VMEM((records, width, width), jnp.bfloat16)]
    else:
        scratch += [pltpu.VMEM(acc_shape, jnp.float32)]
    return pl.pallas_call(
        functools.partial(level_kernel, level, levels, slots, records, packed),
        out_shape=shapes,
        in_specs=in_specs,
        out_specs=[vmem] * len(shapes),
        scratch_shapes=scratch,
        input_output_aliases=aliases,
        compiler_params=pltpu.CompilerParams(vmem_limit_bytes=48 * 1024 * 1024),
        name=f"level_{level}",
    )(*args)


def shards(
    right_side, diag_inverse, off_blocks, live_counts, source_slot, target_owner, target_block
):
    levels, slots, rhs_count, width = right_side.shape
    records = off_blocks.shape[1]
    owners = lax.axis_size(AXES)
    packed = owners * CAP
    order = jnp.arange(records, dtype=jnp.int32)
    same = (target_owner[:, :, None] == target_owner[:, None, :]) & (order[:, None] > order[None, :])
    position = jnp.sum(same.astype(jnp.int32), axis=2)
    slot_of = target_owner * CAP + position
    buffer_ids = jnp.arange(packed, dtype=jnp.int32)
    dummy = levels * slots
    hits = (buffer_ids[None, :, None] == slot_of[:, None, :]).astype(jnp.int32)
    labels = jnp.sum(hits * (target_block - dummy)[:, None, :], axis=2) + dummy
    labels = jnp.swapaxes(labels.reshape(levels - 1, owners, CAP), 0, 1)
    labels = lax.all_to_all(labels, AXES, 0, 0, tiled=True)
    labels = jnp.swapaxes(labels, 0, 1).reshape(levels - 1, packed)
    results = []
    arrived = acc = None
    for level in range(levels):
        last = level == levels - 1
        args = [live_counts]
        if not last:
            args += [source_slot, slot_of]
        if level > 0:
            args += [labels, arrived]
            if level > 1:
                args += [acc]
        args += [right_side, diag_inverse]
        if not last:
            args += [off_blocks]
        out = one_level(level, levels, slots, rhs_count, width, records, packed, args)
        results.append(out[0])
        if not last:
            outgoing = out[1].reshape(owners, CAP * rhs_count, width)
            arrived = lax.all_to_all(outgoing, AXES, 0, 0, tiled=True)
            arrived = arrived.reshape(packed, rhs_count, width)
            if level > 0:
                acc = out[2]
    return jnp.stack(results)


def solution(mesh):
    split = P(None, AXES, None, None)
    flat = P(None, AXES)
    return jax.shard_map(
        shards,
        mesh=mesh,
        in_specs=(split, split, split, flat, flat, flat, flat),
        out_specs=split,
        check_vma=False,
    )
```

```python
import functools

import jax
import jax.numpy as jnp
from jax import lax
from jax.experimental import pallas as pl
from jax.experimental.pallas import tpu as pltpu
from jax.sharding import PartitionSpec as P

CAP = 2
CHAINS = 4
CHUNKS = 8
AXES = ("gx", "gy", "gz")
VMEM = pl.BlockSpec(memory_space=pltpu.VMEM)
HBM = pl.BlockSpec(memory_space=pltpu.HBM)
CONTRACT_LANES = (((1,), (1,)), ((), ()))


def solve(level, rhs, diag, counts, accs, solved):
    slots = solved.shape[0]
    live = jnp.broadcast_to(counts[:, level : level + 1], solved.shape[1:])
    for slot in range(slots):
        work = rhs[slot]
        if accs:
            at = level * slots + slot
            work = work - ((accs[0][at] + accs[1][at]) + (accs[2][at] + accs[3][at]))
        value = jnp.dot(work.astype(jnp.bfloat16), diag[slot], preferred_element_type=jnp.float32)
        solved[slot] = jnp.where(live > slot, value, jnp.float32(0.0))


class Level:
    def __init__(self, level, rhs_hbm, diag_hbm, off_hbm, rhs, diag, off, sems):
        self.parts = [
            pltpu.make_async_copy(rhs_hbm.at[level], rhs, sems.at[0]),
            pltpu.make_async_copy(diag_hbm.at[level], diag, sems.at[1]),
        ]
        self.chunks = []
        if off is not None:
            self.span = off.shape[0] // CHUNKS
            for chunk in range(CHUNKS):
                rows = pl.ds(chunk * self.span, self.span)
                self.chunks.append(
                    pltpu.make_async_copy(off_hbm.at[level, rows], off.at[rows], sems.at[2 + chunk])
                )
        for copy in self.parts + self.chunks:
            copy.start()

    def wait_diagonal(self):
        for copy in self.parts:
            copy.wait()

    def wait_record(self, record):
        if record % self.span == 0:
            self.chunks[record // self.span].wait()


def contribute(loaded, off, solved, source_smem, level, store):
    for record in range(off.shape[0]):
        loaded.wait_record(record)
        picked = solved[source_smem[level, record]].astype(jnp.bfloat16)
        store(record, jnp.dot(picked, off[record], preferred_element_type=jnp.float32))


def first_kernel(
    dummy, counts_hbm, source_hbm, owner_hbm, block_hbm, rhs_hbm, diag_hbm, off_hbm,
    solved, outgoing, slot_table, counts, source, acc_0, acc_1, acc_2, acc_3,
    rhs, diag, off, owner, block, row_vmem, row_smem, source_smem, table_sems, sems,
):
    tables = ((owner_hbm, owner), (block_hbm, block), (counts_hbm, counts), (source_hbm, source))
    tables = [
        pltpu.make_async_copy(table, held, table_sems.at[2 + at])
        for at, (table, held) in enumerate(tables)
    ]
    for copy in tables:
        copy.start()
    source_copy = pltpu.make_async_copy(source_hbm, source_smem, table_sems.at[0])
    row_copy = pltpu.make_async_copy(row_vmem, row_smem, table_sems.at[1])
    source_copy.start()
    loaded = Level(0, rhs_hbm, diag_hbm, off_hbm, rhs, diag, off, sems)
    for acc in (acc_0, acc_1, acc_2, acc_3):
        for row in range(acc.shape[0]):
            acc[row] = jnp.zeros(acc.shape[1:], jnp.float32)
    for copy in tables:
        copy.wait()
    exchanges, width = owner.shape
    owners = width
    stride = outgoing.shape[0] // owners
    height = solved.shape[1]
    down = lax.broadcasted_iota(jnp.int32, (owners, width), 0)
    along = lax.broadcasted_iota(jnp.int32, (owners, width), 1)
    before = (down < along).astype(jnp.bfloat16)
    labels = jnp.full((owners, width), dummy, jnp.float32)
    for level in range(exchanges):
        owner_now = owner[level : level + 1, :]
        hit = (down == owner_now).astype(jnp.float32)
        hit_low = hit.astype(jnp.bfloat16)
        earlier = jnp.dot(hit_low, before, preferred_element_type=jnp.float32)
        position = jnp.sum(hit * earlier, axis=0, keepdims=True)
        place = position.astype(jnp.int32)
        slot_table[level : level + 1, :] = owner_now * CAP + place
        if level == 0:
            row_vmem[...] = owner_now * stride + place * height
            row_copy.start()
        value = (block[level : level + 1, :] - dummy).astype(jnp.float32)
        spread = jnp.where(
            down == CAP * level,
            value * (1.0 - position),
            jnp.where(down == CAP * level + 1, value * position, 0.0),
        ).astype(jnp.bfloat16)
        labels = labels + lax.dot_general(
            hit_low, spread, CONTRACT_LANES, preferred_element_type=jnp.float32
        )
    outgoing[pl.ds(CAP * height, owners, stride=stride), :] = labels
    loaded.wait_diagonal()
    solve(0, rhs, diag, counts, None, solved)
    source_copy.wait()
    row_copy.wait()

    def store(record, value):
        outgoing[pl.ds(row_smem[0, record], height), :] = value

    contribute(loaded, off, solved, source_smem, 0, store)


def later_kernel(level, levels, *refs):
    last = level == levels - 1
    refs = list(refs)
    take = lambda count: [refs.pop(0) for _ in range(count)]
    counts, arrived = take(2)
    accs = take(CHAINS)
    label_table = take(1)[0] if level > 1 else None
    rhs_hbm, diag_hbm = take(2)
    if not last:
        source, slot_table, off_hbm, solved, outgoing = take(5)
        accs = take(CHAINS)
        if level == 1:
            label_table = take(1)[0]
        off, source_smem, slot_smem = take(3)
    else:
        earlier = take(level)
        result, solved = take(2)
        off = off_hbm = None
    rhs, diag, label_smem, table_sems, sems = refs
    height, width = solved.shape[1:]
    owners = label_smem.shape[1]
    stride = arrived.shape[0] // owners
    copies = []
    if level == 1:
        rows = arrived[pl.ds(CAP * height, owners, stride=stride), :].astype(jnp.bfloat16)
        down = lax.broadcasted_iota(jnp.int32, (label_table.shape[0], width), 0)
        along = lax.broadcasted_iota(jnp.int32, (label_table.shape[0], width), 1)
        turned = lax.dot_general(
            (down == along).astype(jnp.bfloat16),
            rows,
            CONTRACT_LANES,
            preferred_element_type=jnp.float32,
        )
        label_table[...] = turned.astype(jnp.int32)
    label_copy = pltpu.make_async_copy(label_table, label_smem, table_sems.at[0])
    label_copy.start()
    loaded = Level(level, rhs_hbm, diag_hbm, off_hbm, rhs, diag, off, sems)
    if not last:
        for at, (table, scalars) in enumerate(((source, source_smem), (slot_table, slot_smem))):
            copies.append(pltpu.make_async_copy(table, scalars, table_sems.at[1 + at]))
    else:
        for at, piece in enumerate(earlier):
            copies.append(pltpu.make_async_copy(piece, result.at[at], table_sems.at[1 + at]))
    for copy in copies:
        copy.start()
    label_copy.wait()
    for sender in range(owners):
        for place in range(CAP):
            acc = accs[(sender % 2) * CAP + place]
            row = label_smem[CAP * (level - 1) + place, sender]
            at = sender * stride + place * height
            acc[row] = acc[row] + arrived[at : at + height, :]
    loaded.wait_diagonal()
    solve(level, rhs, diag, counts, accs, solved)
    if last:
        copy = pltpu.make_async_copy(solved, result.at[level], table_sems.at[1 + level])
        copy.start()
        copies.append(copy)
    for copy in copies:
        copy.wait()
    if not last:

        def store(record, value):
            outgoing[slot_smem[level, record]] = value

        contribute(loaded, off, solved, source_smem, level, store)


def shards(
    right_side, diag_inverse, off_blocks, live_counts, source_slot, target_owner, target_block
):
    levels, slots, height, width = right_side.shape
    exchanges, records = off_blocks.shape[:2]
    owners = lax.axis_size(AXES)
    dummy = levels * slots
    counts = live_counts.T
    stride = CAP * height + 1
    in_hbm = lambda x: pltpu.with_memory_space_constraint(x, pltpu.HBM)
    right_side, diag_inverse, off_blocks = map(in_hbm, (right_side, diag_inverse, off_blocks))
    tables = list(map(in_hbm, (counts, source_slot, target_owner, target_block)))
    table_shape = pltpu.VMEM((exchanges, records), jnp.int32)
    params = pltpu.CompilerParams(vmem_limit_bytes=24 * 1024 * 1024)
    acc_shapes = [pltpu.VMEM((dummy + 1, height, width), jnp.float32)] * CHAINS
    solved_shape = pltpu.VMEM((slots, height, width), jnp.float32)
    level_scratch = [
        pltpu.VMEM((slots, height, width), jnp.float32),
        pltpu.VMEM((slots, width, width), jnp.bfloat16),
    ]
    off_scratch = pltpu.VMEM((records, width, width), jnp.bfloat16)
    table_scratch = pltpu.SMEM((exchanges, records), jnp.int32)
    level_sems = pltpu.SemaphoreType.DMA((2 + CHUNKS,))
    out = pl.pallas_call(
        functools.partial(first_kernel, dummy),
        out_shape=[
            solved_shape,
            pltpu.VMEM((owners * stride, width), jnp.float32),
            table_shape,
            pltpu.VMEM(counts.shape, jnp.int32),
            table_shape,
            *acc_shapes,
        ],
        in_specs=[HBM] * 7,
        out_specs=[VMEM] * (5 + CHAINS),
        scratch_shapes=[
            *level_scratch,
            off_scratch,
            table_shape,
            table_shape,
            pltpu.VMEM((1, records), jnp.int32),
            pltpu.SMEM((1, records), jnp.int32),
            table_scratch,
            pltpu.SemaphoreType.DMA((6,)),
            level_sems,
        ],
        compiler_params=params,
        name="level_0",
    )(*tables, right_side, diag_inverse, off_blocks)
    solved, outgoing, slot_table, counts, source_slot = out[:5]
    accs = out[5:]
    outgoing = outgoing.reshape(owners, stride, 1, width)
    arrived = lax.all_to_all(outgoing, AXES, 0, 0, tiled=True).reshape(owners * stride, width)
    results = [solved]
    label_table = None
    label_shape = (CAP * exchanges, owners)
    for level in range(1, levels):
        last = level == levels - 1
        args = [counts, arrived, *accs]
        specs = [VMEM] * (2 + CHAINS)
        if level > 1:
            args += [label_table]
            specs += [VMEM]
        args += [right_side, diag_inverse]
        specs += [HBM] * 2
        tail = [*level_scratch, pltpu.SMEM(label_shape, jnp.int32)]
        aliases = {}
        if not last:
            args += [source_slot, slot_table, off_blocks]
            specs += [VMEM, VMEM, HBM]
            shapes = [
                solved_shape,
                pltpu.VMEM((owners * CAP, height, width), jnp.float32),
                *acc_shapes,
            ]
            aliases = {2 + chain: 2 + chain for chain in range(CHAINS)}
            if level == 1:
                shapes += [pltpu.VMEM(label_shape, jnp.int32)]
            out_specs = [VMEM] * len(shapes)
            scratch = [off_scratch, table_scratch, table_scratch] + tail
            scratch += [pltpu.SemaphoreType.DMA((3,)), level_sems]
        else:
            args += results
            specs += [VMEM] * level
            shapes = jax.ShapeDtypeStruct((levels, slots, height, width), jnp.float32)
            out_specs = HBM
            scratch = [pltpu.VMEM((slots, height, width), jnp.float32)] + tail
            scratch += [pltpu.SemaphoreType.DMA((2 + level,)), pltpu.SemaphoreType.DMA((2,))]
        out = pl.pallas_call(
            functools.partial(later_kernel, level, levels),
            out_shape=shapes,
            in_specs=specs,
            out_specs=out_specs,
            scratch_shapes=scratch,
            input_output_aliases=aliases,
            compiler_params=params,
            name=f"level_{level}",
        )(*args)
        if last:
            return out
        solved, outgoing = out[:2]
        accs = out[2 : 2 + CHAINS]
        if level == 1:
            label_table = out[2 + CHAINS]
        results.append(solved)
        outgoing = outgoing.reshape(owners, CAP * height, width)
        arrived = lax.all_to_all(outgoing, AXES, 0, 0, tiled=True)
        arrived = arrived.reshape(owners * CAP * height, width)


def solution(mesh):
    split = P(None, AXES, None, None)
    flat = P(None, AXES)
    return jax.shard_map(
        shards,
        mesh=mesh,
        in_specs=(split, split, split, flat, flat, flat, flat),
        out_specs=split,
        check_vma=False,
    )
```

```python
import functools

import jax
import jax.numpy as jnp
from jax import lax
from jax.experimental import pallas as pl
from jax.experimental.pallas import tpu as pltpu
from jax.sharding import PartitionSpec as P

CAP = 2
CHAINS = 4
CHUNKS = 2
AXES = ("gx", "gy", "gz")
VMEM = pl.BlockSpec(memory_space=pltpu.VMEM)
HBM = pl.BlockSpec(memory_space=pltpu.HBM)
CONTRACT_LANES = (((1,), (1,)), ((), ()))


def solve(level, rhs, diag, counts, accs, solved):
    slots = solved.shape[0]
    live = jnp.broadcast_to(counts[:, level : level + 1], solved.shape[1:])
    for slot in range(slots):
        work = rhs[slot]
        if accs:
            at = level * slots + slot
            work = work - ((accs[0][at] + accs[1][at]) + (accs[2][at] + accs[3][at]))
        value = jnp.dot(work.astype(jnp.bfloat16), diag[slot], preferred_element_type=jnp.float32)
        solved[slot] = jnp.where(live > slot, value, jnp.float32(0.0))


class Level:
    def __init__(self, level, sems, pairs, off_hbm=None, off=None, begin=0, chunks=CHUNKS):
        self.parts = [
            pltpu.make_async_copy(source.at[level], held, sems.at[CHUNKS + at])
            for at, (source, held) in enumerate(pairs)
        ]
        self.chunks = []
        self.begin = begin
        if off is not None:
            self.span = off.shape[0] // chunks

            def chunk_copy(chunk):
                rows = pl.ds(chunk * self.span, self.span)
                rows_hbm = pl.ds(begin + chunk * self.span, self.span)
                return pltpu.make_async_copy(
                    off_hbm.at[level, rows_hbm], off.at[rows], sems.at[chunk]
                )

            self.chunk_copy = chunk_copy
            self.chunks = [chunk_copy(chunk) for chunk in range(chunks)]
        for copy in self.parts + self.chunks:
            copy.start()

    def wait_parts(self):
        for copy in self.parts:
            copy.wait()

    def wait_chunk(self, chunk):
        self.chunk_copy(chunk).wait()

    def wait_record(self, record):
        if record >= self.begin and (record - self.begin) % self.span == 0:
            self.chunks[(record - self.begin) // self.span].wait()

    def wait(self):
        for copy in self.parts + self.chunks:
            copy.wait()


def clear(filled):
    for at in range(filled.shape[0]):
        filled[at] = 0


def contribute(loaded, off_of, solved, scalars, filled, level, outgoing, stride, group=None):
    height = solved.shape[1]
    source, owner = scalars

    def one(record):
        picked = solved[source[level, record]].astype(jnp.bfloat16)
        value = jnp.dot(picked, off_of(record), preferred_element_type=jnp.float32)
        to = owner[level, record]
        place = filled[to]
        filled[to] = place + 1
        row = to * stride + place * height
        if stride % height == 0:
            row = pl.multiple_of(row, height)
        outgoing[pl.ds(row, height), :] = value

    records = source.shape[1]
    if group is None:
        for record in range(records):
            if loaded is not None:
                loaded.wait_record(record)
            one(record)
        return

    def several(at, carry):
        if loaded is not None:
            loaded.wait_chunk(at)
        for record in range(group):
            one(at * group + record)
        return carry

    lax.fori_loop(0, records // group, several, 0)


def first_kernel(
    dummy, counts_hbm, source_hbm, owner_hbm, block_hbm, rhs_hbm, diag_hbm, off_hbm,
    solved, outgoing, counts, source, owner, acc_0, acc_1, acc_2, acc_3,
    next_rhs, next_diag, next_off,
    rhs, diag, off, block, source_smem, owner_smem, filled, table_sems, sems, next_sems,
):
    tables = (
        (owner_hbm, owner),
        (block_hbm, block),
        (counts_hbm, counts),
        (source_hbm, source),
        (source_hbm, source_smem),
        (owner_hbm, owner_smem),
    )
    tables = [
        pltpu.make_async_copy(table, held, table_sems.at[at])
        for at, (table, held) in enumerate(tables)
    ]
    for copy in tables:
        copy.start()
    loaded = Level(0, sems, ((rhs_hbm, rhs), (diag_hbm, diag)), off_hbm, off)
    coming = Level(
        1, next_sems, ((rhs_hbm, next_rhs), (diag_hbm, next_diag)), off_hbm, next_off, 0, 1
    )
    clear(filled)
    for acc in (acc_0, acc_1, acc_2, acc_3):
        for row in range(acc.shape[0]):
            acc[row] = jnp.zeros(acc.shape[1:], jnp.float32)
    exchanges, width = owner.shape
    owners = width
    stride = outgoing.shape[0] // owners
    height = solved.shape[1]
    for copy in tables:
        copy.wait()
    loaded.wait_parts()
    solve(0, rhs, diag, counts, None, solved)
    down = lax.broadcasted_iota(jnp.int32, (owners, width), 0)
    along = lax.broadcasted_iota(jnp.int32, (owners, width), 1)
    before = (down < along).astype(jnp.bfloat16)
    labels = jnp.full((owners, width), dummy, jnp.float32)
    for level in range(exchanges):
        hit = (down == owner[level : level + 1, :]).astype(jnp.float32)
        hit_low = hit.astype(jnp.bfloat16)
        earlier = jnp.dot(hit_low, before, preferred_element_type=jnp.float32)
        position = jnp.sum(hit * earlier, axis=0, keepdims=True)
        value = (block[level : level + 1, :] - dummy).astype(jnp.float32)
        spread = jnp.where(
            down == CAP * level,
            value * (1.0 - position),
            jnp.where(down == CAP * level + 1, value * position, 0.0),
        ).astype(jnp.bfloat16)
        labels = labels + lax.dot_general(
            hit_low, spread, CONTRACT_LANES, preferred_element_type=jnp.float32
        )
    outgoing[pl.ds(CAP * height, owners, stride=stride), :] = labels
    off_of = lambda record: off[record]
    contribute(loaded, off_of, solved, (source_smem, owner_smem), filled, 0, outgoing, stride, 64)
    coming.wait()


def later_kernel(level, levels, *refs):
    last = level == levels - 1
    more = level < levels - 2
    refs = list(refs)
    take = lambda count: [refs.pop(0) for _ in range(count)]
    counts, arrived = take(2)
    accs = take(CHAINS)
    label_table = take(1)[0] if level > 1 else None
    rhs, diag = take(2)
    off_hbm = next_off = None
    if not last:
        source, owner, off, rhs_hbm, diag_hbm = take(5)
        if more:
            off_hbm = take(1)[0]
        solved, outgoing = take(2)
        accs = take(CHAINS)
        next_rhs, next_diag = take(2)
        if more:
            next_off = take(1)[0]
        if level == 1:
            label_table, off_rest, rest_sems = take(3)
        source_smem, owner_smem, filled, next_sems = take(4)
    else:
        earlier = take(level)
        result, solved = take(2)
    label_smem, table_sems = refs
    height, width = solved.shape[1:]
    owners = label_smem.shape[1]
    stride = arrived.shape[0] // owners
    rest = None
    if level == 1:
        begin = off.shape[0]
        rest = Level(level, rest_sems, (), off_hbm, off_rest, begin, 2)
        rows = arrived[pl.ds(CAP * height, owners, stride=stride), :].astype(jnp.bfloat16)
        down = lax.broadcasted_iota(jnp.int32, (label_table.shape[0], width), 0)
        along = lax.broadcasted_iota(jnp.int32, (label_table.shape[0], width), 1)
        turned = lax.dot_general(
            (down == along).astype(jnp.bfloat16),
            rows,
            CONTRACT_LANES,
            preferred_element_type=jnp.float32,
        )
        label_table[...] = turned.astype(jnp.int32)
    label_copy = pltpu.make_async_copy(label_table, label_smem, table_sems.at[0])
    label_copy.start()
    copies = []
    if not last:
        for at, (table, scalars) in enumerate(((source, source_smem), (owner, owner_smem))):
            copies.append(pltpu.make_async_copy(table, scalars, table_sems.at[1 + at]))
    else:
        for at, piece in enumerate(earlier):
            copies.append(pltpu.make_async_copy(piece, result.at[at], table_sems.at[1 + at]))
    for copy in copies:
        copy.start()
    if not last:
        coming = Level(
            level + 1,
            next_sems,
            ((rhs_hbm, next_rhs), (diag_hbm, next_diag)),
            off_hbm,
            next_off,
            0,
            1,
        )
        clear(filled)
    label_copy.wait()
    for sender in range(owners):
        for place in range(CAP):
            acc = accs[(sender % 2) * CAP + place]
            row = label_smem[CAP * (level - 1) + place, sender]
            at = sender * stride + place * height
            acc[row] = acc[row] + arrived[at : at + height, :]
    solve(level, rhs, diag, counts, accs, solved)
    if last:
        copy = pltpu.make_async_copy(solved, result.at[level], table_sems.at[1 + level])
        copy.start()
        copies.append(copy)
    for copy in copies:
        copy.wait()
    if not last:
        scalars = (source_smem, owner_smem)
        if rest is None:
            off_of = lambda record: off[record]
        else:
            off_of = lambda record: off[record] if record < begin else off_rest[record - begin]
        contribute(rest, off_of, solved, scalars, filled, level, outgoing, CAP * height)
        coming.wait()


def shards(
    right_side, diag_inverse, off_blocks, live_counts, source_slot, target_owner, target_block
):
    levels, slots, height, width = right_side.shape
    exchanges, records = off_blocks.shape[:2]
    owners = lax.axis_size(AXES)
    dummy = levels * slots
    counts = live_counts.T
    stride = CAP * height + 1
    in_hbm = lambda x: pltpu.with_memory_space_constraint(x, pltpu.HBM)
    right_side, diag_inverse, off_blocks = map(in_hbm, (right_side, diag_inverse, off_blocks))
    tables = list(map(in_hbm, (counts, source_slot, target_owner, target_block)))
    table_shape = pltpu.VMEM((exchanges, records), jnp.int32)
    params = pltpu.CompilerParams(vmem_limit_bytes=24 * 1024 * 1024)
    acc_shapes = [pltpu.VMEM((dummy + 1, height, width), jnp.float32)] * CHAINS
    solved_shape = pltpu.VMEM((slots, height, width), jnp.float32)
    level_shapes = [
        pltpu.VMEM((slots, height, width), jnp.float32),
        pltpu.VMEM((slots, width, width), jnp.bfloat16),
        pltpu.VMEM((records, width, width), jnp.bfloat16),
    ]
    half_shape = pltpu.VMEM((records // 2, width, width), jnp.bfloat16)
    filled_scratch = pltpu.SMEM((owners,), jnp.int32)
    table_scratch = pltpu.SMEM((exchanges, records), jnp.int32)
    level_sems = pltpu.SemaphoreType.DMA((2 + CHUNKS,))
    out = pl.pallas_call(
        functools.partial(first_kernel, dummy),
        out_shape=[
            solved_shape,
            pltpu.VMEM((owners * stride, width), jnp.float32),
            pltpu.VMEM(counts.shape, jnp.int32),
            table_shape,
            table_shape,
            *acc_shapes,
            *level_shapes[:2],
            half_shape,
        ],
        in_specs=[HBM] * 7,
        out_specs=[VMEM] * (8 + CHAINS),
        scratch_shapes=[
            *level_shapes,
            table_shape,
            table_scratch,
            table_scratch,
            filled_scratch,
            pltpu.SemaphoreType.DMA((6,)),
            level_sems,
            level_sems,
        ],
        compiler_params=params,
        name="level_0",
    )(*tables, right_side, diag_inverse, off_blocks)
    solved, outgoing, counts, source_slot, target_owner = out[:5]
    accs = out[5 : 5 + CHAINS]
    held = out[5 + CHAINS :]
    outgoing = outgoing.reshape(owners, stride, 1, width)
    arrived = lax.all_to_all(outgoing, AXES, 0, 0, tiled=True).reshape(owners * stride, width)
    results = [solved]
    label_table = None
    label_shape = (CAP * exchanges, owners)
    for level in range(1, levels):
        last = level == levels - 1
        args = [counts, arrived, *accs]
        specs = [VMEM] * (2 + CHAINS)
        if level > 1:
            args += [label_table]
            specs += [VMEM]
        args += held[:2]
        specs += [VMEM] * 2
        tail = [pltpu.SMEM(label_shape, jnp.int32)]
        aliases = {}
        if not last:
            more = 3 if level < levels - 2 else 2
            args += [source_slot, target_owner, held[2]]
            args += [right_side, diag_inverse, off_blocks][:more]
            specs += [VMEM] * 3 + [HBM] * more
            shapes = [
                solved_shape,
                pltpu.VMEM((owners * CAP * height, width), jnp.float32),
                *acc_shapes,
                *level_shapes[:more],
            ]
            aliases = {2 + chain: 2 + chain for chain in range(CHAINS)}
            if level == 1:
                shapes += [pltpu.VMEM(label_shape, jnp.int32)]
            out_specs = [VMEM] * len(shapes)
            scratch = [table_scratch, table_scratch, filled_scratch, level_sems] + tail
            if level == 1:
                scratch = [half_shape, level_sems] + scratch
            scratch += [pltpu.SemaphoreType.DMA((3,))]
        else:
            args += results
            specs += [VMEM] * level
            shapes = jax.ShapeDtypeStruct((levels, slots, height, width), jnp.float32)
            out_specs = HBM
            scratch = [pltpu.VMEM((slots, height, width), jnp.float32)] + tail
            scratch += [pltpu.SemaphoreType.DMA((2 + level,))]
        out = pl.pallas_call(
            functools.partial(later_kernel, level, levels),
            out_shape=shapes,
            in_specs=specs,
            out_specs=out_specs,
            scratch_shapes=scratch,
            input_output_aliases=aliases,
            compiler_params=params,
            name=f"level_{level}",
        )(*args)
        if last:
            return out
        solved, outgoing = out[:2]
        accs = out[2 : 2 + CHAINS]
        held = out[2 + CHAINS : 2 + CHAINS + more]
        if level == 1:
            label_table = out[2 + CHAINS + more]
        results.append(solved)
        outgoing = outgoing.reshape(owners, CAP * height, width)
        arrived = lax.all_to_all(outgoing, AXES, 0, 0, tiled=True)
        arrived = arrived.reshape(owners * CAP * height, width)


def solution(mesh):
    split = P(None, AXES, None, None)
    flat = P(None, AXES)
    return jax.shard_map(
        shards,
        mesh=mesh,
        in_specs=(split, split, split, flat, flat, flat, flat),
        out_specs=split,
        check_vma=False,
    )
```

```python
import functools

import jax
import jax.numpy as jnp
from jax import lax
from jax.experimental import pallas as pl
from jax.experimental.pallas import tpu as pltpu
from jax.sharding import PartitionSpec as P

CAP = 2
CHAINS = 4
CHUNKS = 2
AXES = ("gx", "gy", "gz")
VMEM = pl.BlockSpec(memory_space=pltpu.VMEM)
HBM = pl.BlockSpec(memory_space=pltpu.HBM)
CONTRACT_LANES = (((1,), (1,)), ((), ()))


def solve(level, rhs, diag, counts, accs, fresh, solved):
    slots = solved.shape[0]
    live = jnp.broadcast_to(counts[:, level : level + 1], solved.shape[1:])
    for slot in range(slots):
        work = rhs[slot]
        if accs:
            at = level * slots + slot
            work = work - ((accs[0][at] + accs[1][at]) + (accs[2][at] + accs[3][at]))
        if fresh is not None:
            height = rhs.shape[1]
            work = work - fresh[slot * height : (slot + 1) * height, :]
        value = jnp.dot(work.astype(jnp.bfloat16), diag[slot], preferred_element_type=jnp.float32)
        solved[slot] = jnp.where(live > slot, value, jnp.float32(0.0))


class Level:
    def __init__(self, level, sems, pairs, off_hbm=None, off=None, begin=0, chunks=CHUNKS):
        self.parts = [
            pltpu.make_async_copy(source.at[level], held, sems.at[CHUNKS + at])
            for at, (source, held) in enumerate(pairs)
        ]
        self.chunks = []
        self.begin = begin
        if off is not None:
            self.span = off.shape[0] // chunks

            def chunk_copy(chunk):
                rows = pl.ds(chunk * self.span, self.span)
                rows_hbm = pl.ds(begin + chunk * self.span, self.span)
                return pltpu.make_async_copy(
                    off_hbm.at[level, rows_hbm], off.at[rows], sems.at[chunk]
                )

            self.chunk_copy = chunk_copy
            self.chunks = [chunk_copy(chunk) for chunk in range(chunks)]
        for copy in self.parts + self.chunks:
            copy.start()

    def wait_parts(self):
        for copy in self.parts:
            copy.wait()

    def wait_chunk(self, chunk):
        self.chunk_copy(chunk).wait()

    def wait_record(self, record):
        if record >= self.begin and (record - self.begin) % self.span == 0:
            self.chunks[(record - self.begin) // self.span].wait()

    def wait(self):
        for copy in self.parts + self.chunks:
            copy.wait()


def clear(filled):
    for at in range(filled.shape[0]):
        filled[at] = 0


def gather_fresh(level, labels, arrived, stride, height, fresh):
    slots = fresh.shape[0] // height
    owners = labels[0].shape[1]
    down = lax.broadcasted_iota(jnp.int32, (slots, owners), 0) + level * slots
    hits = jnp.concatenate([(down == row).astype(jnp.bfloat16) for row in labels], axis=1)
    for row in range(height):
        values = jnp.concatenate(
            [
                arrived[pl.ds(place * height + row, owners, stride=stride), :]
                for place in range(CAP)
            ],
            axis=0,
        )
        high = values.astype(jnp.bfloat16)
        low = (values - high.astype(jnp.float32)).astype(jnp.bfloat16)
        fresh[pl.ds(row, slots, stride=height), :] = jnp.dot(
            hits, high, preferred_element_type=jnp.float32
        ) + jnp.dot(hits, low, preferred_element_type=jnp.float32)


def contribute(loaded, off_of, solved, scalars, filled, level, outgoing, stride, group, beside):
    height = solved.shape[1]
    source, owner = scalars

    def one(record):
        picked = solved[source[level, record]].astype(jnp.bfloat16)
        value = jnp.dot(picked, off_of(record), preferred_element_type=jnp.float32)
        to = owner[level, record]
        place = filled[to]
        filled[to] = place + 1
        row = to * stride + place * height
        if stride % height == 0:
            row = pl.multiple_of(row, height)
        outgoing[pl.ds(row, height), :] = value
        if beside is not None:
            beside(record)

    records = source.shape[1]
    if group is None:
        for record in range(records):
            if loaded is not None:
                loaded.wait_record(record)
            one(record)
        return

    def several(at, carry):
        if loaded is not None:
            loaded.wait_chunk(at)
        for record in range(group):
            one(at * group + record)
        return carry

    lax.fori_loop(0, records // group, several, 0)


def clear_rows(outgoing, stride, height, owners):
    for owner in range(owners):
        for place in range(CAP):
            at = owner * stride + place * height
            outgoing[at : at + height, :] = jnp.zeros((height, outgoing.shape[1]), jnp.float32)


def first_kernel(
    dummy, counts_hbm, source_hbm, owner_hbm, block_hbm, rhs_hbm, diag_hbm, off_hbm,
    solved, outgoing, counts, source, owner,
    rhs, diag, off, block, source_smem, owner_smem, filled, table_sems, sems,
):
    tables = (
        (owner_hbm, owner),
        (block_hbm, block),
        (counts_hbm, counts),
        (source_hbm, source),
        (source_hbm, source_smem),
        (owner_hbm, owner_smem),
    )
    tables = [
        pltpu.make_async_copy(table, held, table_sems.at[at])
        for at, (table, held) in enumerate(tables)
    ]
    for copy in tables:
        copy.start()
    loaded = Level(0, sems, ((rhs_hbm, rhs), (diag_hbm, diag)), off_hbm, off)
    clear(filled)
    exchanges, width = owner.shape
    owners = width
    stride = outgoing.shape[0] // owners
    height = solved.shape[1]
    clear_rows(outgoing, stride, height, owners)
    for copy in tables:
        copy.wait()
    loaded.wait_parts()
    solve(0, rhs, diag, counts, None, None, solved)
    down = lax.broadcasted_iota(jnp.int32, (owners, width), 0)
    along = lax.broadcasted_iota(jnp.int32, (owners, width), 1)
    before = (down < along).astype(jnp.bfloat16)
    labels = jnp.full((owners, width), dummy, jnp.float32)
    for level in range(exchanges):
        hit = (down == owner[level : level + 1, :]).astype(jnp.float32)
        hit_low = hit.astype(jnp.bfloat16)
        earlier = jnp.dot(hit_low, before, preferred_element_type=jnp.float32)
        position = jnp.sum(hit * earlier, axis=0, keepdims=True)
        value = (block[level : level + 1, :] - dummy).astype(jnp.float32)
        spread = jnp.where(
            down == CAP * level,
            value * (1.0 - position),
            jnp.where(down == CAP * level + 1, value * position, 0.0),
        ).astype(jnp.bfloat16)
        labels = labels + lax.dot_general(
            hit_low, spread, CONTRACT_LANES, preferred_element_type=jnp.float32
        )
    outgoing[pl.ds(CAP * height, owners, stride=stride), :] = labels
    off_of = lambda record: off[record]
    contribute(loaded, off_of, solved, (source_smem, owner_smem), filled, 0, outgoing, stride, 64, None)


def later_kernel(level, levels, *refs):
    last = level == levels - 1
    refs = list(refs)
    take = lambda count: [refs.pop(0) for _ in range(count)]
    counts, arrived = take(2)
    accs = take(CHAINS) if level > 1 else []
    label_table = take(1)[0] if level > 1 else None
    rhs, diag = take(2)
    if not last:
        source, owner, off, solved, outgoing = take(5)
        next_accs = take(CHAINS)
        if level == 1:
            label_table = take(1)[0]
        source_smem, owner_smem, label_smem, filled = take(4)
    else:
        earlier = take(level)
        result, solved = take(2)
    fresh, fence, table_sems = refs
    height, width = solved.shape[1:]
    owners = width
    stride = arrived.shape[0] // owners
    if not last:
        tables = [(source, source_smem), (owner, owner_smem)]
        if level > 1:
            tables += [(label_table, label_smem)]
    else:
        tables = [(piece, result.at[at]) for at, piece in enumerate(earlier)]
    copies = [
        pltpu.make_async_copy(table, held, table_sems.at[at])
        for at, (table, held) in enumerate(tables)
    ]
    for copy in copies:
        copy.start()
    pl.semaphore_signal(fence, 1)
    pl.semaphore_wait(fence, 1)
    if level == 1:
        rows = arrived[pl.ds(CAP * height, owners, stride=stride), :].astype(jnp.bfloat16)
        down = lax.broadcasted_iota(jnp.int32, (label_table.shape[0], width), 0)
        along = lax.broadcasted_iota(jnp.int32, (label_table.shape[0], width), 1)
        turned = lax.dot_general(
            (down == along).astype(jnp.bfloat16),
            rows,
            CONTRACT_LANES,
            preferred_element_type=jnp.float32,
        )
        label_table[...] = turned.astype(jnp.int32)
        label_copy = pltpu.make_async_copy(label_table, label_smem, table_sems.at[2])
        label_copy.start()
        copies.append(label_copy)
    if not last:
        clear(filled)
        clear_rows(outgoing, CAP * height, height, owners)
    first_label = CAP * (level - 1)
    labels = [label_table[first_label + place : first_label + place + 1, :] for place in range(CAP)]
    gather_fresh(level, labels, arrived, stride, height, fresh)
    solve(level, rhs.at[level], diag.at[level], counts, accs, fresh, solved)
    if last:
        copy = pltpu.make_async_copy(solved, result.at[level], table_sems.at[level])
        copy.start()
        copies.append(copy)
        for copy in copies:
            copy.wait()
        return
    if level == 1:
        for acc in next_accs:
            for row in range((level + 1) * solved.shape[0], acc.shape[0]):
                acc[row] = jnp.zeros(acc.shape[1:], jnp.float32)
    for copy in copies:
        copy.wait()

    def accumulate(sender):
        for place in range(CAP):
            acc = next_accs[(sender % 2) * CAP + place]
            row = label_smem[first_label + place, sender]
            at = sender * stride + place * height
            acc[row] = acc[row] + arrived[at : at + height, :]

    off_of = lambda record: off[level, record]
    scalars = (source_smem, owner_smem)
    contribute(
        None, off_of, solved, scalars, filled, level, outgoing, CAP * height, None, accumulate
    )


def shards(
    right_side, diag_inverse, off_blocks, live_counts, source_slot, target_owner, target_block
):
    levels, slots, height, width = right_side.shape
    exchanges, records = off_blocks.shape[:2]
    owners = lax.axis_size(AXES)
    dummy = levels * slots
    counts = live_counts.T
    stride = CAP * height + 1
    in_hbm = lambda x: pltpu.with_memory_space_constraint(x, pltpu.HBM)
    tables = list(map(in_hbm, (counts, source_slot, target_owner, target_block)))
    table_shape = pltpu.VMEM((exchanges, records), jnp.int32)
    params = pltpu.CompilerParams(vmem_limit_bytes=24 * 1024 * 1024)
    acc_shapes = [pltpu.VMEM((dummy + 1, height, width), jnp.float32)] * CHAINS
    solved_shape = pltpu.VMEM((slots, height, width), jnp.float32)
    level_shapes = [
        pltpu.VMEM((slots, height, width), jnp.float32),
        pltpu.VMEM((slots, width, width), jnp.bfloat16),
        pltpu.VMEM((records, width, width), jnp.bfloat16),
    ]
    filled_scratch = pltpu.SMEM((owners,), jnp.int32)
    table_scratch = pltpu.SMEM((exchanges, records), jnp.int32)
    level_sems = pltpu.SemaphoreType.DMA((2 + CHUNKS,))
    out = pl.pallas_call(
        functools.partial(first_kernel, dummy),
        out_shape=[
            solved_shape,
            pltpu.VMEM((owners * stride, width), jnp.float32),
            pltpu.VMEM(counts.shape, jnp.int32),
            table_shape,
            table_shape,
        ],
        in_specs=[HBM] * 7,
        out_specs=[VMEM] * 5,
        scratch_shapes=[
            *level_shapes,
            table_shape,
            table_scratch,
            table_scratch,
            filled_scratch,
            pltpu.SemaphoreType.DMA((6,)),
            level_sems,
        ],
        compiler_params=params,
        name="level_0",
    )(*tables, *map(in_hbm, (right_side, diag_inverse, off_blocks)))
    solved, outgoing, counts, source_slot, target_owner = out[:5]
    accs = []
    in_vmem = lambda x: pltpu.with_memory_space_constraint(x, pltpu.VMEM)
    held = list(map(in_vmem, (right_side, diag_inverse, off_blocks)))
    outgoing = outgoing.reshape(owners, stride, 1, width)
    arrived = lax.all_to_all(outgoing, AXES, 0, 0, tiled=True).reshape(owners * stride, width)
    results = [solved]
    label_table = None
    label_shape = (CAP * exchanges, owners)
    for level in range(1, levels):
        last = level == levels - 1
        args = [counts, arrived, *accs]
        specs = [VMEM] * len(args)
        if level > 1:
            args += [label_table]
            specs += [VMEM]
        args += held[:2]
        specs += [VMEM] * 2
        tail = [
            pltpu.VMEM((slots * height, width), jnp.float32),
            pltpu.SemaphoreType.REGULAR,
        ]
        aliases = {}
        if not last:
            args += [source_slot, target_owner, held[2]]
            specs += [VMEM] * 3
            shapes = [
                solved_shape,
                pltpu.VMEM((owners * CAP * height, width), jnp.float32),
                *acc_shapes,
            ]
            aliases = {2 + chain: 2 + chain for chain in range(len(accs))}
            if level == 1:
                shapes += [pltpu.VMEM(label_shape, jnp.int32)]
            out_specs = [VMEM] * len(shapes)
            label_scratch = pltpu.SMEM(label_shape, jnp.int32)
            scratch = [table_scratch, table_scratch, label_scratch, filled_scratch] + tail
            scratch += [pltpu.SemaphoreType.DMA((3,))]
        else:
            args += results
            specs += [VMEM] * level
            shapes = jax.ShapeDtypeStruct((levels, slots, height, width), jnp.float32)
            out_specs = HBM
            scratch = [pltpu.VMEM((slots, height, width), jnp.float32)] + tail
            scratch += [pltpu.SemaphoreType.DMA((2 + level,))]
        out = pl.pallas_call(
            functools.partial(later_kernel, level, levels),
            out_shape=shapes,
            in_specs=specs,
            out_specs=out_specs,
            scratch_shapes=scratch,
            input_output_aliases=aliases,
            compiler_params=params,
            name=f"level_{level}",
        )(*args)
        if last:
            return out
        solved, outgoing = out[:2]
        accs = out[2 : 2 + CHAINS]
        if level == 1:
            label_table = out[2 + CHAINS]
        results.append(solved)
        outgoing = outgoing.reshape(owners, CAP * height, width)
        arrived = lax.all_to_all(outgoing, AXES, 0, 0, tiled=True)
        arrived = arrived.reshape(owners * CAP * height, width)


def solution(mesh):
    split = P(None, AXES, None, None)
    flat = P(None, AXES)
    return jax.shard_map(
        shards,
        mesh=mesh,
        in_specs=(split, split, split, flat, flat, flat, flat),
        out_specs=split,
        check_vma=False,
    )
```

```python
import functools

import jax
import jax.numpy as jnp
from jax import lax
from jax.experimental import pallas as pl
from jax.experimental.pallas import tpu as pltpu
from jax.sharding import PartitionSpec as P

CAP = 2
CHAINS = 4
STARTS = (0, 64)
AXES = ("gx", "gy", "gz")
VMEM = pl.BlockSpec(memory_space=pltpu.VMEM)
HBM = pl.BlockSpec(memory_space=pltpu.HBM)
CONTRACT_LANES = (((1,), (1,)), ((), ()))


def solve(level, rhs, diag, counts, accs, fresh, solved):
    slots = solved.shape[0]
    live = jnp.broadcast_to(counts[:, level : level + 1], solved.shape[1:])
    for slot in range(slots):
        work = rhs[slot]
        if accs:
            at = level * slots + slot
            work = work - ((accs[0][at] + accs[1][at]) + (accs[2][at] + accs[3][at]))
        if fresh is not None:
            height = rhs.shape[1]
            work = work - fresh[slot * height : (slot + 1) * height, :]
        value = jnp.dot(work.astype(jnp.bfloat16), diag[slot], preferred_element_type=jnp.float32)
        solved[slot] = jnp.where(live > slot, value, jnp.float32(0.0))


class Level:
    def __init__(self, level, sems, pairs, off_hbm, off):
        self.parts = [
            pltpu.make_async_copy(source.at[level], held, sems.at[at])
            for at, (source, held) in enumerate(pairs)
        ]
        edges = [*STARTS, off.shape[0]]
        self.chunks = {}
        for at, begin in enumerate(STARTS):
            rows = pl.ds(begin, edges[at + 1] - begin)
            self.chunks[begin] = pltpu.make_async_copy(
                off_hbm.at[level, rows], off.at[rows], sems.at[len(pairs) + at]
            )
        for copy in [*self.parts, *self.chunks.values()]:
            copy.start()

    def wait_parts(self):
        for copy in self.parts:
            copy.wait()

    def wait_record(self, record):
        if record in self.chunks:
            self.chunks[record].wait()


def clear(filled):
    for at in range(filled.shape[0]):
        filled[at] = 0


def gather_fresh(level, labels, arrived, stride, height, fresh):
    slots = fresh.shape[0] // height
    owners = labels[0].shape[1]
    down = lax.broadcasted_iota(jnp.int32, (slots, owners), 0) + level * slots
    hits = jnp.concatenate([(down == row).astype(jnp.bfloat16) for row in labels], axis=1)
    for row in range(height):
        values = jnp.concatenate(
            [
                arrived[pl.ds(place * height + row, owners, stride=stride), :]
                for place in range(CAP)
            ],
            axis=0,
        )
        high = values.astype(jnp.bfloat16)
        low = (values - high.astype(jnp.float32)).astype(jnp.bfloat16)
        fresh[pl.ds(row, slots, stride=height), :] = jnp.dot(
            hits, high, preferred_element_type=jnp.float32
        ) + jnp.dot(hits, low, preferred_element_type=jnp.float32)


def contribute(loaded, off_of, solved, scalars, filled, level, outgoing, stride, beside):
    height = solved.shape[1]
    source, owner = scalars

    def one(record):
        picked = solved[source[level, record]].astype(jnp.bfloat16)
        value = jnp.dot(picked, off_of(record), preferred_element_type=jnp.float32)
        to = owner[level, record]
        place = filled[to]
        filled[to] = place + 1
        row = to * stride + place * height
        if stride % height == 0:
            row = pl.multiple_of(row, height)
        outgoing[pl.ds(row, height), :] = value
        if beside is not None:
            beside(record)

    records = source.shape[1]
    for record in range(records):
        if loaded is not None:
            loaded.wait_record(record)
        one(record)


def clear_rows(outgoing, stride, height, owners):
    for owner in range(owners):
        for place in range(CAP):
            at = owner * stride + place * height
            outgoing[at : at + height, :] = jnp.zeros((height, outgoing.shape[1]), jnp.float32)


def first_kernel(
    dummy, counts_hbm, source_hbm, owner_hbm, block_hbm, rhs_hbm, diag_hbm, off_hbm,
    solved, outgoing, counts, source, owner,
    rhs, diag, off, block, source_smem, owner_smem, filled, table_sems, sems,
):
    tables = (
        (owner_hbm, owner),
        (block_hbm, block),
        (counts_hbm, counts),
        (source_hbm, source),
        (source_hbm, source_smem),
        (owner_hbm, owner_smem),
    )
    tables = [
        pltpu.make_async_copy(table, held, table_sems.at[at])
        for at, (table, held) in enumerate(tables)
    ]
    for copy in tables:
        copy.start()
    loaded = Level(0, sems, ((rhs_hbm, rhs), (diag_hbm, diag)), off_hbm, off)
    clear(filled)
    exchanges, width = owner.shape
    owners = width
    stride = outgoing.shape[0] // owners
    height = solved.shape[1]
    clear_rows(outgoing, stride, height, owners)
    for copy in tables:
        copy.wait()
    loaded.wait_parts()
    solve(0, rhs, diag, counts, None, None, solved)
    down = lax.broadcasted_iota(jnp.int32, (owners, width), 0)
    along = lax.broadcasted_iota(jnp.int32, (owners, width), 1)
    before = (down < along).astype(jnp.bfloat16)
    labels = jnp.full((owners, width), dummy, jnp.float32)
    for level in range(exchanges):
        hit = (down == owner[level : level + 1, :]).astype(jnp.float32)
        hit_low = hit.astype(jnp.bfloat16)
        earlier = jnp.dot(hit_low, before, preferred_element_type=jnp.float32)
        position = jnp.sum(hit * earlier, axis=0, keepdims=True)
        value = (block[level : level + 1, :] - dummy).astype(jnp.float32)
        spread = jnp.where(
            down == CAP * level,
            value * (1.0 - position),
            jnp.where(down == CAP * level + 1, value * position, 0.0),
        ).astype(jnp.bfloat16)
        labels = labels + lax.dot_general(
            hit_low, spread, CONTRACT_LANES, preferred_element_type=jnp.float32
        )
    outgoing[pl.ds(CAP * height, owners, stride=stride), :] = labels
    off_of = lambda record: off[record]
    contribute(loaded, off_of, solved, (source_smem, owner_smem), filled, 0, outgoing, stride, None)


def later_kernel(level, levels, *refs):
    last = level == levels - 1
    refs = list(refs)
    take = lambda count: [refs.pop(0) for _ in range(count)]
    counts, arrived = take(2)
    accs = take(CHAINS) if level > 1 else []
    label_table = take(1)[0] if level > 1 else None
    rhs, diag = take(2)
    if not last:
        source, owner, off, solved, outgoing = take(5)
        next_accs = take(CHAINS)
        if level == 1:
            label_table = take(1)[0]
        source_smem, owner_smem, label_smem, filled = take(4)
    else:
        earlier = take(level)
        result, solved = take(2)
    fresh, fence, table_sems = refs
    height, width = solved.shape[1:]
    owners = width
    stride = arrived.shape[0] // owners
    if not last:
        tables = [(source, source_smem), (owner, owner_smem)]
        if level > 1:
            tables += [(label_table, label_smem)]
    else:
        tables = [(piece, result.at[at]) for at, piece in enumerate(earlier)]
    copies = [
        pltpu.make_async_copy(table, held, table_sems.at[at])
        for at, (table, held) in enumerate(tables)
    ]
    for copy in copies:
        copy.start()
    pl.semaphore_signal(fence, 1)
    pl.semaphore_wait(fence, 1)
    if level == 1:
        rows = arrived[pl.ds(CAP * height, owners, stride=stride), :].astype(jnp.bfloat16)
        down = lax.broadcasted_iota(jnp.int32, (label_table.shape[0], width), 0)
        along = lax.broadcasted_iota(jnp.int32, (label_table.shape[0], width), 1)
        turned = lax.dot_general(
            (down == along).astype(jnp.bfloat16),
            rows,
            CONTRACT_LANES,
            preferred_element_type=jnp.float32,
        )
        label_table[...] = turned.astype(jnp.int32)
        label_copy = pltpu.make_async_copy(label_table, label_smem, table_sems.at[2])
        label_copy.start()
        copies.append(label_copy)
    if not last:
        clear(filled)
        clear_rows(outgoing, CAP * height, height, owners)
    first_label = CAP * (level - 1)
    labels = [label_table[first_label + place : first_label + place + 1, :] for place in range(CAP)]
    gather_fresh(level, labels, arrived, stride, height, fresh)
    solve(level, rhs.at[level], diag.at[level], counts, accs, fresh, solved)
    if last:
        copy = pltpu.make_async_copy(solved, result.at[level], table_sems.at[level])
        copy.start()
        copies.append(copy)
        for copy in copies:
            copy.wait()
        return
    if level == 1:
        for acc in next_accs:
            for row in range((level + 1) * solved.shape[0], acc.shape[0]):
                acc[row] = jnp.zeros(acc.shape[1:], jnp.float32)
    for copy in copies:
        copy.wait()

    def accumulate(sender):
        for place in range(CAP):
            acc = next_accs[(sender % 2) * CAP + place]
            row = label_smem[first_label + place, sender]
            at = sender * stride + place * height
            acc[row] = acc[row] + arrived[at : at + height, :]

    off_of = lambda record: off[level, record]
    scalars = (source_smem, owner_smem)
    contribute(
        None, off_of, solved, scalars, filled, level, outgoing, CAP * height, accumulate
    )


def shards(
    right_side, diag_inverse, off_blocks, live_counts, source_slot, target_owner, target_block
):
    levels, slots, height, width = right_side.shape
    exchanges, records = off_blocks.shape[:2]
    owners = lax.axis_size(AXES)
    dummy = levels * slots
    counts = live_counts.T
    stride = CAP * height + 1
    in_hbm = lambda x: pltpu.with_memory_space_constraint(x, pltpu.HBM)
    tables = list(map(in_hbm, (counts, source_slot, target_owner, target_block)))
    table_shape = pltpu.VMEM((exchanges, records), jnp.int32)
    later_params = pltpu.CompilerParams(
        vmem_limit_bytes=24 * 1024 * 1024,
    )
    params = pltpu.CompilerParams(vmem_limit_bytes=24 * 1024 * 1024)
    acc_shapes = [pltpu.VMEM((dummy + 1, height, width), jnp.float32)] * CHAINS
    solved_shape = pltpu.VMEM((slots, height, width), jnp.float32)
    level_shapes = [
        pltpu.VMEM((slots, height, width), jnp.float32),
        pltpu.VMEM((slots, width, width), jnp.bfloat16),
        pltpu.VMEM((records, width, width), jnp.bfloat16),
    ]
    filled_scratch = pltpu.SMEM((owners,), jnp.int32)
    table_scratch = pltpu.SMEM((exchanges, records), jnp.int32)
    level_sems = pltpu.SemaphoreType.DMA((2 + len(STARTS),))
    out = pl.pallas_call(
        functools.partial(first_kernel, dummy),
        out_shape=[
            solved_shape,
            pltpu.VMEM((owners * stride, width), jnp.float32),
            pltpu.VMEM(counts.shape, jnp.int32),
            table_shape,
            table_shape,
        ],
        in_specs=[HBM] * 7,
        out_specs=[VMEM] * 5,
        scratch_shapes=[
            *level_shapes,
            table_shape,
            table_scratch,
            table_scratch,
            filled_scratch,
            pltpu.SemaphoreType.DMA((6,)),
            level_sems,
        ],
        compiler_params=params,
        name="level_0",
    )(*tables, *map(in_hbm, (right_side, diag_inverse, off_blocks)))
    solved, outgoing, counts, source_slot, target_owner = out[:5]
    accs = []
    in_vmem = lambda x: pltpu.with_memory_space_constraint(x, pltpu.VMEM)
    held = list(map(in_vmem, (right_side, diag_inverse, off_blocks)))
    outgoing = outgoing.reshape(owners, stride, 1, width)
    arrived = lax.all_to_all(outgoing, AXES, 0, 0, tiled=True).reshape(owners * stride, width)
    results = [solved]
    label_table = None
    label_shape = (CAP * exchanges, owners)
    for level in range(1, levels):
        last = level == levels - 1
        args = [counts, arrived, *accs]
        specs = [VMEM] * len(args)
        if level > 1:
            args += [label_table]
            specs += [VMEM]
        args += held[:2]
        specs += [VMEM] * 2
        tail = [
            pltpu.VMEM((slots * height, width), jnp.float32),
            pltpu.SemaphoreType.REGULAR,
        ]
        aliases = {}
        if not last:
            args += [source_slot, target_owner, held[2]]
            specs += [VMEM] * 3
            shapes = [
                solved_shape,
                pltpu.VMEM((owners * CAP * height, width), jnp.float32),
                *acc_shapes,
            ]
            aliases = {2 + chain: 2 + chain for chain in range(len(accs))}
            if level == 1:
                shapes += [pltpu.VMEM(label_shape, jnp.int32)]
            out_specs = [VMEM] * len(shapes)
            label_scratch = pltpu.SMEM(label_shape, jnp.int32)
            scratch = [table_scratch, table_scratch, label_scratch, filled_scratch] + tail
            scratch += [pltpu.SemaphoreType.DMA((3,))]
        else:
            args += results
            specs += [VMEM] * level
            shapes = jax.ShapeDtypeStruct((levels, slots, height, width), jnp.float32)
            out_specs = HBM
            scratch = [pltpu.VMEM((slots, height, width), jnp.float32)] + tail
            scratch += [pltpu.SemaphoreType.DMA((2 + level,))]
        out = pl.pallas_call(
            functools.partial(later_kernel, level, levels),
            out_shape=shapes,
            in_specs=specs,
            out_specs=out_specs,
            scratch_shapes=scratch,
            input_output_aliases=aliases,
            compiler_params=later_params,
            name=f"level_{level}",
        )(*args)
        if last:
            return out
        solved, outgoing = out[:2]
        accs = out[2 : 2 + CHAINS]
        if level == 1:
            label_table = out[2 + CHAINS]
        results.append(solved)
        outgoing = outgoing.reshape(owners, CAP * height, width)
        arrived = lax.all_to_all(outgoing, AXES, 0, 0, tiled=True)
        arrived = arrived.reshape(owners * CAP * height, width)


def solution(mesh):
    split = P(None, AXES, None, None)
    flat = P(None, AXES)
    return jax.shard_map(
        shards,
        mesh=mesh,
        in_specs=(split, split, split, flat, flat, flat, flat),
        out_specs=split,
        check_vma=False,
    )
```

```python
import functools

import jax
import jax.numpy as jnp
from jax import lax
from jax.experimental import pallas as pl
from jax.experimental.pallas import tpu as pltpu
from jax.sharding import PartitionSpec as P

CAP = 2
CHAINS = 2
STARTS = (0, 64)
AXES = ("gx", "gy", "gz")
VMEM = pl.BlockSpec(memory_space=pltpu.VMEM)
HBM = pl.BlockSpec(memory_space=pltpu.HBM)
CONTRACT_LANES = (((1,), (1,)), ((), ()))


def solve(level, rhs, diag, counts, accs, fresh, solved):
    slots = solved.shape[0]
    live = jnp.broadcast_to(counts[:, level : level + 1], solved.shape[1:])
    for slot in range(slots):
        work = rhs[slot]
        if accs:
            at = level * slots + slot
            work = work - sum(acc[at] for acc in accs)
        if fresh is not None:
            height = rhs.shape[1]
            work = work - fresh[slot * height : (slot + 1) * height, :]
        value = jnp.dot(work.astype(jnp.bfloat16), diag[slot], preferred_element_type=jnp.float32)
        solved[slot] = jnp.where(live > slot, value, jnp.float32(0.0))


class Level:
    def __init__(self, level, sems, pairs, off_hbm, off):
        self.parts = [
            pltpu.make_async_copy(source.at[level], held, sems.at[at])
            for at, (source, held) in enumerate(pairs)
        ]
        edges = [*STARTS, off.shape[0]]
        self.chunks = {}
        for at, begin in enumerate(STARTS):
            rows = pl.ds(begin, edges[at + 1] - begin)
            self.chunks[begin] = pltpu.make_async_copy(
                off_hbm.at[level, rows], off.at[rows], sems.at[len(pairs) + at]
            )
        for copy in [*self.parts, *self.chunks.values()]:
            copy.start()

    def wait_parts(self):
        for copy in self.parts:
            copy.wait()

    def wait_record(self, record):
        if record in self.chunks:
            self.chunks[record].wait()


def clear(filled):
    for at in range(filled.shape[0]):
        filled[at] = 0


def gather_fresh(level, labels, arrived, stride, height, fresh):
    slots = fresh.shape[0] // height
    owners = labels[0].shape[1]
    down = lax.broadcasted_iota(jnp.int32, (slots, owners), 0) + level * slots
    hits = jnp.concatenate([(down == row).astype(jnp.bfloat16) for row in labels], axis=1)
    for row in range(height):
        values = jnp.concatenate(
            [
                arrived[pl.ds(place * height + row, owners, stride=stride), :]
                for place in range(CAP)
            ],
            axis=0,
        )
        high = values.astype(jnp.bfloat16)
        low = (values - high.astype(jnp.float32)).astype(jnp.bfloat16)
        fresh[pl.ds(row, slots, stride=height), :] = jnp.dot(
            hits, high, preferred_element_type=jnp.float32
        ) + jnp.dot(hits, low, preferred_element_type=jnp.float32)


def contribute(loaded, off_of, solved, scalars, filled, level, outgoing, stride, beside):
    height = solved.shape[1]
    source, owner = scalars

    def one(record):
        picked = solved[source[level, record]].astype(jnp.bfloat16)
        value = jnp.dot(picked, off_of(record), preferred_element_type=jnp.float32)
        to = owner[level, record]
        place = filled[to]
        filled[to] = place + 1
        row = to * stride + place * height
        if stride % height == 0:
            row = pl.multiple_of(row, height)
        outgoing[pl.ds(row, height), :] = value
        if beside is not None:
            beside(record)

    records = source.shape[1]
    for record in range(records):
        if loaded is not None:
            loaded.wait_record(record)
        one(record)


def clear_rows(outgoing, stride, height, owners):
    for owner in range(owners):
        for place in range(CAP):
            at = owner * stride + place * height
            outgoing[at : at + height, :] = jnp.zeros((height, outgoing.shape[1]), jnp.float32)


def first_kernel(
    dummy, counts_hbm, source_hbm, owner_hbm, block_hbm, rhs_hbm, diag_hbm, off_hbm,
    solved, outgoing, counts, source, owner,
    rhs, diag, off, block, source_smem, owner_smem, filled, table_sems, sems,
):
    tables = (
        (owner_hbm, owner),
        (block_hbm, block),
        (counts_hbm, counts),
        (source_hbm, source),
        (source_hbm, source_smem),
        (owner_hbm, owner_smem),
    )
    tables = [
        pltpu.make_async_copy(table, held, table_sems.at[at])
        for at, (table, held) in enumerate(tables)
    ]
    for copy in tables:
        copy.start()
    loaded = Level(0, sems, ((rhs_hbm, rhs), (diag_hbm, diag)), off_hbm, off)
    clear(filled)
    exchanges, width = owner.shape
    owners = width
    stride = outgoing.shape[0] // owners
    height = solved.shape[1]
    clear_rows(outgoing, stride, height, owners)
    for copy in tables:
        copy.wait()
    loaded.wait_parts()
    solve(0, rhs, diag, counts, None, None, solved)
    down = lax.broadcasted_iota(jnp.int32, (owners, width), 0)
    along = lax.broadcasted_iota(jnp.int32, (owners, width), 1)
    before = (down < along).astype(jnp.bfloat16)
    labels = jnp.full((owners, width), dummy, jnp.float32)
    for level in range(exchanges):
        hit = (down == owner[level : level + 1, :]).astype(jnp.float32)
        hit_low = hit.astype(jnp.bfloat16)
        earlier = jnp.dot(hit_low, before, preferred_element_type=jnp.float32)
        position = jnp.sum(hit * earlier, axis=0, keepdims=True)
        value = (block[level : level + 1, :] - dummy).astype(jnp.float32)
        spread = jnp.where(
            down == CAP * level,
            value * (1.0 - position),
            jnp.where(down == CAP * level + 1, value * position, 0.0),
        ).astype(jnp.bfloat16)
        labels = labels + lax.dot_general(
            hit_low, spread, CONTRACT_LANES, preferred_element_type=jnp.float32
        )
    outgoing[pl.ds(CAP * height, owners, stride=stride), :] = labels
    off_of = lambda record: off[record]
    contribute(loaded, off_of, solved, (source_smem, owner_smem), filled, 0, outgoing, stride, None)


def later_kernel(level, levels, *refs):
    last = level == levels - 1
    refs = list(refs)
    take = lambda count: [refs.pop(0) for _ in range(count)]
    counts, arrived = take(2)
    accs = take(CHAINS) if level > 1 else []
    label_table = take(1)[0] if level > 1 else None
    rhs, diag = take(2)
    if not last:
        source, owner, off, solved, outgoing = take(5)
        next_accs = take(CHAINS)
        if level == 1:
            label_table = take(1)[0]
        source_smem, owner_smem, label_smem, filled = take(4)
    else:
        earlier = take(level)
        result, solved = take(2)
    fresh, fence, table_sems = refs
    height, width = solved.shape[1:]
    owners = width
    stride = arrived.shape[0] // owners
    if not last:
        tables = [(source, source_smem), (owner, owner_smem)]
        if level > 1:
            tables += [(label_table, label_smem)]
    else:
        tables = [(piece, result.at[at]) for at, piece in enumerate(earlier)]
    copies = [
        pltpu.make_async_copy(table, held, table_sems.at[at])
        for at, (table, held) in enumerate(tables)
    ]
    for copy in copies:
        copy.start()
    pl.semaphore_signal(fence, 1)
    pl.semaphore_wait(fence, 1)
    if level == 1:
        rows = arrived[pl.ds(CAP * height, owners, stride=stride), :].astype(jnp.bfloat16)
        down = lax.broadcasted_iota(jnp.int32, (label_table.shape[0], width), 0)
        along = lax.broadcasted_iota(jnp.int32, (label_table.shape[0], width), 1)
        turned = lax.dot_general(
            (down == along).astype(jnp.bfloat16),
            rows,
            CONTRACT_LANES,
            preferred_element_type=jnp.float32,
        )
        label_table[...] = turned.astype(jnp.int32)
        label_copy = pltpu.make_async_copy(label_table, label_smem, table_sems.at[2])
        label_copy.start()
        copies.append(label_copy)
    if not last:
        clear(filled)
        clear_rows(outgoing, CAP * height, height, owners)
    first_label = CAP * (level - 1)
    labels = [label_table[first_label + place : first_label + place + 1, :] for place in range(CAP)]
    gather_fresh(level, labels, arrived, stride, height, fresh)
    solve(level, rhs.at[level], diag.at[level], counts, accs, fresh, solved)
    if last:
        copy = pltpu.make_async_copy(solved, result.at[level], table_sems.at[level])
        copy.start()
        copies.append(copy)
        for copy in copies:
            copy.wait()
        return
    if level == 1:
        for acc in next_accs:
            for row in range((level + 1) * solved.shape[0], acc.shape[0]):
                acc[row] = jnp.zeros(acc.shape[1:], jnp.float32)
    for copy in copies:
        copy.wait()

    def accumulate(sender):
        for place in range(CAP):
            acc = next_accs[(sender * CAP + place) % CHAINS]
            row = label_smem[first_label + place, sender]
            at = sender * stride + place * height
            acc[row] = acc[row] + arrived[at : at + height, :]

    off_of = lambda record: off[level, record]
    scalars = (source_smem, owner_smem)
    contribute(
        None, off_of, solved, scalars, filled, level, outgoing, CAP * height, accumulate
    )


def shards(
    right_side, diag_inverse, off_blocks, live_counts, source_slot, target_owner, target_block
):
    levels, slots, height, width = right_side.shape
    exchanges, records = off_blocks.shape[:2]
    owners = lax.axis_size(AXES)
    dummy = levels * slots
    counts = live_counts.T
    stride = CAP * height + 1
    in_hbm = lambda x: pltpu.with_memory_space_constraint(x, pltpu.HBM)
    tables = list(map(in_hbm, (counts, source_slot, target_owner, target_block)))
    table_shape = pltpu.VMEM((exchanges, records), jnp.int32)
    later_params = pltpu.CompilerParams(
        vmem_limit_bytes=24 * 1024 * 1024,
    )
    params = pltpu.CompilerParams(vmem_limit_bytes=24 * 1024 * 1024)
    acc_shapes = [pltpu.VMEM((dummy + 1, height, width), jnp.float32)] * CHAINS
    solved_shape = pltpu.VMEM((slots, height, width), jnp.float32)
    level_shapes = [
        pltpu.VMEM((slots, height, width), jnp.float32),
        pltpu.VMEM((slots, width, width), jnp.bfloat16),
        pltpu.VMEM((records, width, width), jnp.bfloat16),
    ]
    filled_scratch = pltpu.SMEM((owners,), jnp.int32)
    table_scratch = pltpu.SMEM((exchanges, records), jnp.int32)
    level_sems = pltpu.SemaphoreType.DMA((2 + len(STARTS),))
    out = pl.pallas_call(
        functools.partial(first_kernel, dummy),
        out_shape=[
            solved_shape,
            pltpu.VMEM((owners * stride, width), jnp.float32),
            pltpu.VMEM(counts.shape, jnp.int32),
            table_shape,
            table_shape,
        ],
        in_specs=[HBM] * 7,
        out_specs=[VMEM] * 5,
        scratch_shapes=[
            *level_shapes,
            table_shape,
            table_scratch,
            table_scratch,
            filled_scratch,
            pltpu.SemaphoreType.DMA((6,)),
            level_sems,
        ],
        compiler_params=params,
        name="level_0",
    )(*tables, *map(in_hbm, (right_side, diag_inverse, off_blocks)))
    solved, outgoing, counts, source_slot, target_owner = out[:5]
    accs = []
    in_vmem = lambda x: pltpu.with_memory_space_constraint(x, pltpu.VMEM)
    held = list(map(in_vmem, (right_side, diag_inverse, off_blocks)))
    outgoing = outgoing.reshape(owners, stride, 1, width)
    arrived = lax.all_to_all(outgoing, AXES, 0, 0, tiled=True).reshape(owners * stride, width)
    results = [solved]
    label_table = None
    label_shape = (CAP * exchanges, owners)
    for level in range(1, levels):
        last = level == levels - 1
        args = [counts, arrived, *accs]
        specs = [VMEM] * len(args)
        if level > 1:
            args += [label_table]
            specs += [VMEM]
        args += held[:2]
        specs += [VMEM] * 2
        tail = [
            pltpu.VMEM((slots * height, width), jnp.float32),
            pltpu.SemaphoreType.REGULAR,
        ]
        aliases = {}
        if not last:
            args += [source_slot, target_owner, held[2]]
            specs += [VMEM] * 3
            shapes = [
                solved_shape,
                pltpu.VMEM((owners * CAP * height, width), jnp.float32),
                *acc_shapes,
            ]
            aliases = {2 + chain: 2 + chain for chain in range(len(accs))}
            if level == 1:
                shapes += [pltpu.VMEM(label_shape, jnp.int32)]
            out_specs = [VMEM] * len(shapes)
            label_scratch = pltpu.SMEM(label_shape, jnp.int32)
            scratch = [table_scratch, table_scratch, label_scratch, filled_scratch] + tail
            scratch += [pltpu.SemaphoreType.DMA((3,))]
        else:
            args += results
            specs += [VMEM] * level
            shapes = jax.ShapeDtypeStruct((levels, slots, height, width), jnp.float32)
            out_specs = HBM
            scratch = [pltpu.VMEM((slots, height, width), jnp.float32)] + tail
            scratch += [pltpu.SemaphoreType.DMA((2 + level,))]
        out = pl.pallas_call(
            functools.partial(later_kernel, level, levels),
            out_shape=shapes,
            in_specs=specs,
            out_specs=out_specs,
            scratch_shapes=scratch,
            input_output_aliases=aliases,
            compiler_params=later_params,
            name=f"level_{level}",
        )(*args)
        if last:
            return out
        solved, outgoing = out[:2]
        accs = out[2 : 2 + CHAINS]
        if level == 1:
            label_table = out[2 + CHAINS]
        results.append(solved)
        outgoing = outgoing.reshape(owners, CAP * height, width)
        arrived = lax.all_to_all(outgoing, AXES, 0, 0, tiled=True)
        arrived = arrived.reshape(owners * CAP * height, width)


def solution(mesh):
    split = P(None, AXES, None, None)
    flat = P(None, AXES)
    return jax.shard_map(
        shards,
        mesh=mesh,
        in_specs=(split, split, split, flat, flat, flat, flat),
        out_specs=split,
        check_vma=False,
    )
```

```python
import functools

import jax
import jax.numpy as jnp
from jax import lax
from jax.experimental import pallas as pl
from jax.experimental.pallas import tpu as pltpu
from jax.sharding import PartitionSpec as P

CAP = 2
CHAINS = 2
STARTS = (0, 64)
AXES = ("gx", "gy", "gz")
VMEM = pl.BlockSpec(memory_space=pltpu.VMEM)
HBM = pl.BlockSpec(memory_space=pltpu.HBM)
CONTRACT_LANES = (((1,), (1,)), ((), ()))


def solve(level, rhs, diag, counts, accs, fresh, solved, part=0, parts=1):
    slots = solved.shape[0]
    live = jnp.broadcast_to(counts[:, level : level + 1], solved.shape[1:])
    for slot in range(part * slots // parts, (part + 1) * slots // parts):
        work = rhs[slot]
        if accs:
            at = level * slots + slot
            work = work - sum(acc[at] for acc in accs)
        if fresh is not None:
            height = rhs.shape[1]
            work = work - fresh[slot * height : (slot + 1) * height, :]
        value = jnp.dot(work.astype(jnp.bfloat16), diag[slot], preferred_element_type=jnp.float32)
        solved[slot] = jnp.where(live > slot, value, jnp.float32(0.0))


class Level:
    def __init__(self, level, sems, pairs, off_hbm, off):
        self.parts = [
            pltpu.make_async_copy(source.at[level], held, sems.at[at])
            for at, (source, held) in enumerate(pairs)
        ]
        edges = [*STARTS, off.shape[0]]
        self.chunks = {}
        for at, begin in enumerate(STARTS):
            rows = pl.ds(begin, edges[at + 1] - begin)
            self.chunks[begin] = pltpu.make_async_copy(
                off_hbm.at[level, rows], off.at[rows], sems.at[len(pairs) + at]
            )
        for copy in [*self.parts, *self.chunks.values()]:
            copy.start()

    def wait_parts(self):
        for copy in self.parts:
            copy.wait()

    def wait_record(self, record):
        if record in self.chunks:
            self.chunks[record].wait()


def clear(filled):
    for at in range(filled.shape[0]):
        filled[at] = 0


def gather_fresh(level, labels, arrived, stride, height, fresh):
    slots = fresh.shape[0] // height
    owners = labels[0].shape[1]
    down = lax.broadcasted_iota(jnp.int32, (slots, owners), 0) + level * slots
    hits = jnp.concatenate([(down == row).astype(jnp.bfloat16) for row in labels], axis=1)
    for row in range(height):
        values = jnp.concatenate(
            [
                arrived[pl.ds(place * height + row, owners, stride=stride), :]
                for place in range(CAP)
            ],
            axis=0,
        )
        high = values.astype(jnp.bfloat16)
        low = (values - high.astype(jnp.float32)).astype(jnp.bfloat16)
        fresh[pl.ds(row, slots, stride=height), :] = jnp.dot(
            hits, high, preferred_element_type=jnp.float32
        ) + jnp.dot(hits, low, preferred_element_type=jnp.float32)


def contribute(loaded, off_of, solved, scalars, filled, level, outgoing, stride, beside):
    height = solved.shape[1]
    source, owner = scalars

    def one(record):
        picked = solved[source[level, record]].astype(jnp.bfloat16)
        value = jnp.dot(picked, off_of(record), preferred_element_type=jnp.float32)
        to = owner[level, record]
        place = filled[to]
        filled[to] = place + 1
        row = to * stride + place * height
        if stride % height == 0:
            row = pl.multiple_of(row, height)
        outgoing[pl.ds(row, height), :] = value
        if beside is not None:
            beside(record)

    records = source.shape[1]
    for record in range(records):
        if loaded is not None:
            loaded.wait_record(record)
        one(record)


def clear_rows(outgoing, stride, height, owners):
    for owner in range(owners):
        for place in range(CAP):
            at = owner * stride + place * height
            outgoing[at : at + height, :] = jnp.zeros((height, outgoing.shape[1]), jnp.float32)


def first_kernel(
    dummy, counts_hbm, source_hbm, owner_hbm, block_hbm, rhs_hbm, diag_hbm, off_hbm,
    solved, outgoing, counts, source, owner,
    rhs, diag, off, block, source_smem, owner_smem, filled, table_sems, sems,
):
    tables = (
        (owner_hbm, owner),
        (block_hbm, block),
        (counts_hbm, counts),
        (source_hbm, source),
        (source_hbm, source_smem),
        (owner_hbm, owner_smem),
    )
    tables = [
        pltpu.make_async_copy(table, held, table_sems.at[at])
        for at, (table, held) in enumerate(tables)
    ]
    for copy in tables:
        copy.start()
    loaded = Level(0, sems, ((rhs_hbm, rhs), (diag_hbm, diag)), off_hbm, off)
    clear(filled)
    exchanges, width = owner.shape
    owners = width
    stride = outgoing.shape[0] // owners
    height = solved.shape[1]
    clear_rows(outgoing, stride, height, owners)
    for copy in tables:
        copy.wait()
    loaded.wait_parts()
    solve(0, rhs, diag, counts, None, None, solved)
    down = lax.broadcasted_iota(jnp.int32, (owners, width), 0)
    along = lax.broadcasted_iota(jnp.int32, (owners, width), 1)
    before = (down < along).astype(jnp.bfloat16)
    labels = jnp.full((owners, width), dummy, jnp.float32)
    for level in range(exchanges):
        hit = (down == owner[level : level + 1, :]).astype(jnp.float32)
        hit_low = hit.astype(jnp.bfloat16)
        earlier = jnp.dot(hit_low, before, preferred_element_type=jnp.float32)
        position = jnp.sum(hit * earlier, axis=0, keepdims=True)
        value = (block[level : level + 1, :] - dummy).astype(jnp.float32)
        spread = jnp.where(
            down == CAP * level,
            value * (1.0 - position),
            jnp.where(down == CAP * level + 1, value * position, 0.0),
        ).astype(jnp.bfloat16)
        labels = labels + lax.dot_general(
            hit_low, spread, CONTRACT_LANES, preferred_element_type=jnp.float32
        )
    outgoing[pl.ds(CAP * height, owners, stride=stride), :] = labels
    off_of = lambda record: off[record]
    contribute(loaded, off_of, solved, (source_smem, owner_smem), filled, 0, outgoing, stride, None)


def later_kernel(level, levels, *refs):
    last = level == levels - 1
    refs = list(refs)
    take = lambda count: [refs.pop(0) for _ in range(count)]
    counts, arrived = take(2)
    accs = take(CHAINS) if level > 1 else []
    label_table = take(1)[0] if level > 1 else None
    rhs, diag = take(2)
    if not last:
        source, owner, off, solved, outgoing = take(5)
        next_accs = take(CHAINS)
        if level == 1:
            label_table = take(1)[0]
        source_smem, owner_smem, label_smem, filled = take(4)
    else:
        earlier = take(level)
        result, solved = take(2)
    fresh, fence, table_sems = refs
    height, width = solved.shape[1:]
    owners = width
    stride = arrived.shape[0] // owners
    if not last:
        tables = [(source, source_smem), (owner, owner_smem)]
        if level > 1:
            tables += [(label_table, label_smem)]
    else:
        tables = [(piece, result.at[at]) for at, piece in enumerate(earlier)]
    copies = [
        pltpu.make_async_copy(table, held, table_sems.at[at])
        for at, (table, held) in enumerate(tables)
    ]
    for copy in copies:
        copy.start()
    pl.semaphore_signal(fence, 1)
    pl.semaphore_wait(fence, 1)
    if level == 1:
        rows = arrived[pl.ds(CAP * height, owners, stride=stride), :].astype(jnp.bfloat16)
        down = lax.broadcasted_iota(jnp.int32, (label_table.shape[0], width), 0)
        along = lax.broadcasted_iota(jnp.int32, (label_table.shape[0], width), 1)
        turned = lax.dot_general(
            (down == along).astype(jnp.bfloat16),
            rows,
            CONTRACT_LANES,
            preferred_element_type=jnp.float32,
        )
        label_table[...] = turned.astype(jnp.int32)
        label_copy = pltpu.make_async_copy(label_table, label_smem, table_sems.at[2])
        label_copy.start()
        copies.append(label_copy)
    if not last:
        clear(filled)
        clear_rows(outgoing, CAP * height, height, owners)
    first_label = CAP * (level - 1)
    labels = [label_table[first_label + place : first_label + place + 1, :] for place in range(CAP)]
    gather_fresh(level, labels, arrived, stride, height, fresh)
    if last:
        half = solved.shape[0] // 2
        for part in range(2):
            solve(level, rhs.at[level], diag.at[level], counts, accs, fresh, solved, part, 2)
            rows = pl.ds(part * half, half)
            copy = pltpu.make_async_copy(
                solved.at[rows], result.at[level, rows], table_sems.at[level + part]
            )
            copy.start()
            copies.append(copy)
        for copy in copies:
            copy.wait()
        return
    solve(level, rhs.at[level], diag.at[level], counts, accs, fresh, solved)
    if level == 1:
        for acc in next_accs:
            for row in range((level + 1) * solved.shape[0], acc.shape[0]):
                acc[row] = jnp.zeros(acc.shape[1:], jnp.float32)
    for copy in copies:
        copy.wait()

    def accumulate(sender):
        for place in range(CAP):
            acc = next_accs[(sender * CAP + place) % CHAINS]
            row = label_smem[first_label + place, sender]
            at = sender * stride + place * height
            acc[row] = acc[row] + arrived[at : at + height, :]

    off_of = lambda record: off[level, record]
    scalars = (source_smem, owner_smem)
    contribute(
        None, off_of, solved, scalars, filled, level, outgoing, CAP * height, accumulate
    )


def shards(
    right_side, diag_inverse, off_blocks, live_counts, source_slot, target_owner, target_block
):
    levels, slots, height, width = right_side.shape
    exchanges, records = off_blocks.shape[:2]
    owners = lax.axis_size(AXES)
    dummy = levels * slots
    counts = live_counts.T
    stride = CAP * height + 1
    in_hbm = lambda x: pltpu.with_memory_space_constraint(x, pltpu.HBM)
    tables = list(map(in_hbm, (counts, source_slot, target_owner, target_block)))
    table_shape = pltpu.VMEM((exchanges, records), jnp.int32)
    later_params = pltpu.CompilerParams(
        vmem_limit_bytes=24 * 1024 * 1024,
    )
    params = pltpu.CompilerParams(vmem_limit_bytes=24 * 1024 * 1024)
    acc_shapes = [pltpu.VMEM((dummy + 1, height, width), jnp.float32)] * CHAINS
    solved_shape = pltpu.VMEM((slots, height, width), jnp.float32)
    level_shapes = [
        pltpu.VMEM((slots, height, width), jnp.float32),
        pltpu.VMEM((slots, width, width), jnp.bfloat16),
        pltpu.VMEM((records, width, width), jnp.bfloat16),
    ]
    filled_scratch = pltpu.SMEM((owners,), jnp.int32)
    table_scratch = pltpu.SMEM((exchanges, records), jnp.int32)
    level_sems = pltpu.SemaphoreType.DMA((2 + len(STARTS),))
    out = pl.pallas_call(
        functools.partial(first_kernel, dummy),
        out_shape=[
            solved_shape,
            pltpu.VMEM((owners * stride, width), jnp.float32),
            pltpu.VMEM(counts.shape, jnp.int32),
            table_shape,
            table_shape,
        ],
        in_specs=[HBM] * 7,
        out_specs=[VMEM] * 5,
        scratch_shapes=[
            *level_shapes,
            table_shape,
            table_scratch,
            table_scratch,
            filled_scratch,
            pltpu.SemaphoreType.DMA((6,)),
            level_sems,
        ],
        compiler_params=params,
        name="level_0",
    )(*tables, *map(in_hbm, (right_side, diag_inverse, off_blocks)))
    solved, outgoing, counts, source_slot, target_owner = out[:5]
    accs = []
    in_vmem = lambda x: pltpu.with_memory_space_constraint(x, pltpu.VMEM)
    held = list(map(in_vmem, (right_side, diag_inverse, off_blocks)))
    outgoing = outgoing.reshape(owners, stride, 1, width)
    arrived = lax.all_to_all(outgoing, AXES, 0, 0, tiled=True).reshape(owners * stride, width)
    results = [solved]
    label_table = None
    label_shape = (CAP * exchanges, owners)
    for level in range(1, levels):
        last = level == levels - 1
        args = [counts, arrived, *accs]
        specs = [VMEM] * len(args)
        if level > 1:
            args += [label_table]
            specs += [VMEM]
        args += held[:2]
        specs += [VMEM] * 2
        tail = [
            pltpu.VMEM((slots * height, width), jnp.float32),
            pltpu.SemaphoreType.REGULAR,
        ]
        aliases = {}
        if not last:
            args += [source_slot, target_owner, held[2]]
            specs += [VMEM] * 3
            shapes = [
                solved_shape,
                pltpu.VMEM((owners * CAP * height, width), jnp.float32),
                *acc_shapes,
            ]
            aliases = {2 + chain: 2 + chain for chain in range(len(accs))}
            if level == 1:
                shapes += [pltpu.VMEM(label_shape, jnp.int32)]
            out_specs = [VMEM] * len(shapes)
            label_scratch = pltpu.SMEM(label_shape, jnp.int32)
            scratch = [table_scratch, table_scratch, label_scratch, filled_scratch] + tail
            scratch += [pltpu.SemaphoreType.DMA((3,))]
        else:
            args += results
            specs += [VMEM] * level
            shapes = jax.ShapeDtypeStruct((levels, slots, height, width), jnp.float32)
            out_specs = HBM
            scratch = [pltpu.VMEM((slots, height, width), jnp.float32)] + tail
            scratch += [pltpu.SemaphoreType.DMA((2 + level,))]
        out = pl.pallas_call(
            functools.partial(later_kernel, level, levels),
            out_shape=shapes,
            in_specs=specs,
            out_specs=out_specs,
            scratch_shapes=scratch,
            input_output_aliases=aliases,
            compiler_params=later_params,
            name=f"level_{level}",
        )(*args)
        if last:
            return out
        solved, outgoing = out[:2]
        accs = out[2 : 2 + CHAINS]
        if level == 1:
            label_table = out[2 + CHAINS]
        results.append(solved)
        outgoing = outgoing.reshape(owners, CAP * height, width)
        arrived = lax.all_to_all(outgoing, AXES, 0, 0, tiled=True)
        arrived = arrived.reshape(owners * CAP * height, width)


def solution(mesh):
    split = P(None, AXES, None, None)
    flat = P(None, AXES)
    return jax.shard_map(
        shards,
        mesh=mesh,
        in_specs=(split, split, split, flat, flat, flat, flat),
        out_specs=split,
        check_vma=False,
    )
```
